32 devices in a mesh: neg: 8 (over y, x, core), qry: 4 (over z).
Axes of the slice: x: 2, y: 2, z: 4, core: 2. Of those that a mesh axis runs over, the one named last changes fastest.
Arguments:
- items_table: bfloat16 [65536, 512], P('neg'), may hold values from -6 to 6
- fetch_rows: int32 [256, 1280], P(('neg', 'qry')), may hold values from 0 to 8191, as said below
- neighbour_slots: int32 [16384, 40], P(('neg', 'qry')), may hold values from 0 to 10239, as said below
- neighbour_count: int32 [16384], P(('neg', 'qry')), may hold values from 20 to 40
- self_slot: int32 [16384], P(('neg', 'qry')), may hold values from 0 to 10239
- negative_count: int32 [16384], P('neg'), may hold values from 1 to 999
- message_weight: bfloat16 [512, 512], replicated, may hold values from -0.25 to 0.25
- message_bias: float32 [512], replicated, may hold values from -3 to 3
- self_weight: bfloat16 [512, 512], replicated, may hold values from -0.25 to 0.25
- neighbour_weight: bfloat16 [512, 512], replicated, may hold values from -0.25 to 0.25
- output_bias: float32 [512], replicated, may hold values from -3 to 3
- queries: bfloat16 [4096, 512], P('qry'), may hold values from -8 to 8
Outputs:
- negative_embed: bfloat16 [16384, 512], P(('neg', 'qry'))
- query_lse: float32 [4096], P('qry')
The draws below stay inside these ranges and needn't reach their ends.
Inputs may be any that keep to these rules, and one draw needn't show every extreme that they name: Within one row of fetch_rows (one device's list for one partition) no item appears twice. `neighbour_slots`: every one of a device's 8 * 1280 fetched rows is named by at least one live neighbour of that device's negatives.
All inputs are finite; a program needn't handle non-finite values.
Results may differ from the reference program's by a relative error of at most 0.0055.
Values may be sent and summed in bfloat16 or wider, within the bound.
A program may use at most 128 MiB of HBM per device.

```python
import math
import jax
import jax.numpy as jnp
from jax import lax

D = 512
K = 40
ITEM_DEV = 8192
NEG_DEV = 512
CAP = 1280
NEG = 16384
QRY = 4096
ITEMS = 65536
N_NEG = 8
N_QRY = 4


def draw_queries(key, part):
    values = jnp.clip(jax.random.normal(key, (QRY, D), jnp.float32), -5.5, 5.5)
    return values.astype(jnp.bfloat16)


def draw_fetch_rows(key, part):
    row_keys = jax.random.split(jax.random.fold_in(key, 7), N_NEG * N_QRY * N_NEG)

    def one_row(row_key):
        return jax.random.permutation(row_key, ITEM_DEV)[:CAP].astype(jnp.int32)
    return jax.vmap(one_row)(row_keys).astype(jnp.int32)


def neighbour_draw(key):
    count_key = jax.random.fold_in(key, 11)
    counts = jax.random.randint(count_key, (NEG,), K // 2, K + 1, dtype=jnp.int32)
    slot_total = N_NEG * CAP
    device_keys = jax.random.split(jax.random.fold_in(key, 13), N_NEG * N_QRY)
    count_blocks = counts.reshape(N_NEG * N_QRY, NEG_DEV)

    def one_device(device_key, count_block):
        order_key = jax.random.fold_in(device_key, 1)
        filler_key = jax.random.fold_in(device_key, 2)
        live_mask = jnp.arange(K, dtype=jnp.int32)[None, :] < count_block[:, None]
        priority = jax.random.randint(order_key, (NEG_DEV * K,), 0, 1 << 20, dtype=jnp.int32)
        priority = priority + jnp.where(live_mask.reshape(-1), 0, 1 << 21).astype(jnp.int32)
        order = jnp.argsort(priority, stable=True).astype(jnp.int32)
        ranked = jnp.argsort(order, stable=True).astype(jnp.int32)
        filler = jax.random.randint(filler_key, (NEG_DEV * K,), 0, slot_total, dtype=jnp.int32)
        slots = jnp.where(ranked < slot_total, ranked, filler)
        return slots.reshape(NEG_DEV, K).astype(jnp.int32)
    slots = jax.vmap(one_device)(device_keys, count_blocks).reshape(NEG, K)
    return (counts, slots)


def draw_neighbour_count(key, part):
    return neighbour_draw(key)[0].astype(jnp.int32)


def draw_neighbour_slots(key, part):
    return neighbour_draw(key)[1].astype(jnp.int32)


def place_ends(drawn, stream_key, smallest, largest):
    longest = drawn.shape.index(max(drawn.shape))
    spots = []
    for shift in (0, 1):
        where = [jax.random.randint(jax.random.fold_in(stream_key, axis), (), 0, length) for axis, length in enumerate(drawn.shape)]
        where[longest] = (where[longest] + shift) % drawn.shape[longest]
        spots.append(tuple(where))
    return drawn.at[spots[0]].set(smallest).at[spots[1]].set(largest)


def shard_levels(own_key, shape, cuts, least, high):
    factor_of = 1.0
    for dim, parts in cuts:
        draws = jax.random.uniform(jax.random.fold_in(jax.random.fold_in(own_key, 6), dim), (parts,), jnp.float32, least / len(cuts), high / len(cuts))
        factor_of = factor_of * jnp.repeat(jnp.exp(draws), shape[dim] // parts).reshape((-1,) + (1,) * (len(shape) - 1 - dim))
    return factor_of


def gaussian(key, shape, deviation, limit, pieces=(), kind=jnp.bfloat16):
    factor_of = shard_levels(key, shape, pieces, -0.22, 0.18) if pieces else 1.0
    values = jax.random.normal(key, shape, jnp.float32) * deviation * factor_of
    return jnp.minimum(jnp.maximum(values, -limit), limit).astype(kind)


def setup_inputs(seed: int = 0) -> dict:
    seeds = jax.random.split(jax.random.key(seed), 13)
    items_table = gaussian(seeds[0], (ITEMS, D), 1.0, 6.0, ((0, 8),))
    fetch_rows = draw_fetch_rows(jax.random.fold_in(seeds[12], 71), 0)
    neighbour_slots = draw_neighbour_slots(jax.random.fold_in(seeds[12], 71), 0)
    neighbour_count = draw_neighbour_count(jax.random.fold_in(seeds[12], 71), 0)
    self_slot = place_ends(jax.random.randint(seeds[4], (NEG,), 0, N_NEG * CAP), jax.random.fold_in(seeds[4], 1), 0, (N_NEG * CAP) - 1).astype(jnp.int32)
    negative_count = place_ends(jax.random.randint(seeds[5], (NEG,), 1, 1000), jax.random.fold_in(seeds[5], 1), 1, 999).astype(jnp.int32)
    message_weight = gaussian(seeds[6], (D, D), D ** -0.5, 0.25)
    message_bias = gaussian(seeds[7], (D,), 0.5, 3.0, (), jnp.float32)
    self_weight = gaussian(seeds[8], (D, D), D ** -0.5, 0.25)
    neighbour_weight = gaussian(seeds[9], (D, D), D ** -0.5, 0.25)
    output_bias = gaussian(seeds[10], (D,), 0.5, 3.0, (), jnp.float32)
    queries = draw_queries(jax.random.fold_in(seeds[12], 71), 0)
    return {"items_table": items_table, "fetch_rows": fetch_rows, "neighbour_slots": neighbour_slots, "neighbour_count": neighbour_count, "self_slot": self_slot, "negative_count": negative_count, "message_weight": message_weight, "message_bias": message_bias, "self_weight": self_weight, "neighbour_weight": neighbour_weight, "output_bias": output_bias, "queries": queries}


def embed_device(items_table, fetch_block, slot_block, count_block, self_block, message_weight, message_bias, self_weight, neighbour_weight, output_bias):
    owners = jnp.arange(N_NEG, dtype=jnp.int32)[:, None] * ITEM_DEV
    global_rows = (fetch_block.astype(jnp.int32) + owners).reshape(-1)
    fetched = items_table[global_rows]
    message = jax.nn.relu(jnp.dot(fetched, message_weight, preferred_element_type=jnp.float32) + message_bias).astype(jnp.bfloat16)
    gathered = message[slot_block].astype(jnp.float32)
    live_mask = jnp.arange(K, dtype=jnp.int32)[None, :] < count_block[:, None]
    summed = lax.optimization_barrier(jnp.sum(jnp.where(live_mask[:, :, None], gathered, jnp.float32(0.0)), axis=1))
    neighbour_mean = (summed / count_block.astype(jnp.float32)[:, None]).astype(jnp.bfloat16)
    self_rows = fetched[self_block]
    hidden = jnp.dot(self_rows, self_weight, preferred_element_type=jnp.float32)
    hidden = hidden + jnp.dot(neighbour_mean, neighbour_weight, preferred_element_type=jnp.float32) + output_bias
    hidden = jax.nn.relu(hidden)
    scale_inv = lax.rsqrt(lax.optimization_barrier(jnp.mean(hidden * hidden, axis=-1, keepdims=True)) + 0.25)
    return (hidden * scale_inv).astype(jnp.bfloat16)

def reference(items_table, fetch_rows, neighbour_slots, neighbour_count, self_slot, negative_count, message_weight, message_bias, self_weight, neighbour_weight, output_bias, queries):
    devices_all = N_NEG * N_QRY
    fetch_all = fetch_rows.reshape(devices_all, N_NEG, -1)
    slots_all = neighbour_slots.reshape(devices_all, -1, K)
    counts_all = neighbour_count.reshape(devices_all, -1)
    selves_all = self_slot.reshape(devices_all, -1)

    def one_device(inputs):
        return embed_device(items_table, inputs[0], inputs[1], inputs[2], inputs[3], message_weight, message_bias, self_weight, neighbour_weight, output_bias)
    embedded = lax.map(one_device, (fetch_all, slots_all, counts_all, selves_all))
    negative_embed = embedded.reshape(-1, D)
    log_count = jnp.log(negative_count.astype(jnp.float32))
    query_blocks = queries.reshape(N_QRY, -1, D)

    def one_block(query_block):
        scores = 0.25 * jnp.dot(query_block, negative_embed.T, preferred_element_type=jnp.float32) - log_count[None, :]
        peak = lax.optimization_barrier(jnp.max(scores, axis=1))
        totals = lax.optimization_barrier(jnp.sum(jnp.exp(scores - peak[:, None]), axis=1))
        return peak + jnp.log(totals) - math.log(NEG)
    query_lse = lax.map(one_block, query_blocks).reshape(-1)
    return (negative_embed, query_lse)
```

```python
import functools
import math

import jax
import jax.numpy as jnp
from jax import lax
from jax.experimental import pallas as pl
from jax.experimental.pallas import tpu as pltpu
from jax.sharding import PartitionSpec as P


LANES = 128
ROWS = 128
NT = (((1,), (1,)), ((), ()))


def sort_pairs(count):
    full = 1
    while full < count:
        full *= 2
    pairs = []
    p = 1
    while p < full:
        k = p
        while k >= 1:
            for j in range(k % p, full - k, 2 * k):
                for i in range(min(k, full - j - k)):
                    if (i + j) // (2 * p) == (i + j + k) // (2 * p):
                        if i + j + k < count:
                            pairs.append((i + j, i + j + k))
            k //= 2
        p *= 2
    return pairs


def partial_kernel(
    base_ref, rows_ref, slots_ref, self_ref, wm_ref, mb_ref, ws_ref, wn_ref,
    out_ref, order_ref, times_ref, counts_ref, self_hot_ref,
):
    cap = rows_ref.shape[1]
    neighbours, groups = slots_ref.shape[1], slots_ref.shape[2]
    big = jnp.int32(1 << 28)
    base = base_ref[0]
    places = []
    live = jnp.zeros((groups, LANES), jnp.int32)
    mine = jnp.zeros((groups, LANES), jnp.int32)
    for k in range(neighbours):
        slot = slots_ref[0, k]
        local = slot - base
        inside = (local >= 0) & (local < cap) & (slot >= 0)
        live = live + jnp.where(slot >= 0, 1, 0)
        mine = mine + jnp.where(inside, 1, 0)
        places.append(jnp.where(inside, local, big))
    for a, b in sort_pairs(neighbours):
        low, high = jnp.minimum(places[a], places[b]), jnp.maximum(places[a], places[b])
        places[a], places[b] = low, high
    run = jnp.ones((groups, LANES), jnp.float32)
    for k in range(neighbours):
        if k:
            run = jnp.where(places[k] == places[k - 1], run + 1.0, 1.0)
        order_ref[k] = places[k]
        times_ref[k] = run
    longest = jnp.max(mine)
    steps = (longest + 1) // 2
    inverse = 1.0 / live.astype(jnp.float32)
    iota = lax.broadcasted_iota(jnp.int32, (ROWS, LANES), 0)
    self_local = self_ref[0] - base
    for g in range(groups):
        lanes = pl.ds(g * LANES, LANES)

        @pl.loop(0, cap // ROWS)
        def _(c):
            first = c * ROWS
            here = iota + first

            def step(i, total):
                for u in range(2):
                    k = 2 * i + u
                    slot = order_ref[k, pl.ds(g, 1), :]
                    total = jnp.where(here == slot, times_ref[k, pl.ds(g, 1), :], total)
                return total

            total = lax.fori_loop(0, steps, step, jnp.zeros((ROWS, LANES), jnp.float32))
            span = pl.ds(pl.multiple_of(first, ROWS), ROWS)
            counts_ref[span, lanes] = total.astype(jnp.bfloat16)
            self_hot_ref[span, lanes] = jnp.where(
                here == self_local[g : g + 1, :], 1.0, 0.0
            ).astype(jnp.bfloat16)

    rows = rows_ref[0]
    message = jax.nn.relu(
        lax.dot_general(wm_ref[...], rows, NT, preferred_element_type=jnp.float32) + mb_ref[...]
    ).astype(jnp.bfloat16)
    summed = jnp.dot(message, counts_ref[...], preferred_element_type=jnp.float32)
    scale = jnp.concatenate([inverse[g : g + 1, :] for g in range(groups)], axis=1)
    mean = (summed * scale).astype(jnp.bfloat16)
    own = lax.dot_general(ws_ref[...], rows, NT, preferred_element_type=jnp.float32).astype(
        jnp.bfloat16
    )
    part = jnp.dot(own, self_hot_ref[...], preferred_element_type=jnp.float32)
    part = part + jnp.dot(wn_ref[...], mean, preferred_element_type=jnp.float32)
    out_ref[0] = part.astype(jnp.bfloat16)


def partial_hidden(base, rows, slots, selves, wm, mb, ws, wn):
    blocks, cap, width = rows.shape
    neighbours, groups = slots.shape[1], slots.shape[2]
    negatives = groups * LANES
    whole = pl.BlockSpec(memory_space=pltpu.VMEM)
    return pl.pallas_call(
        partial_kernel,
        grid=(blocks,),
        out_shape=jax.ShapeDtypeStruct((blocks, width, negatives), jnp.bfloat16),
        in_specs=[
            pl.BlockSpec(memory_space=pltpu.SMEM),
            pl.BlockSpec((1, cap, width), lambda b: (b, 0, 0)),
            pl.BlockSpec((1, neighbours, groups, LANES), lambda b: (b, 0, 0, 0)),
            pl.BlockSpec((1, groups, LANES), lambda b: (b, 0, 0)),
            whole, whole, whole, whole,
        ],
        out_specs=pl.BlockSpec((1, width, negatives), lambda b: (b, 0, 0)),
        scratch_shapes=[
            pltpu.VMEM((neighbours, groups, LANES), jnp.int32),
            pltpu.VMEM((neighbours, groups, LANES), jnp.float32),
            pltpu.VMEM((cap, negatives), jnp.bfloat16),
            pltpu.VMEM((cap, negatives), jnp.bfloat16),
        ],
        cost_estimate=pl.CostEstimate(
            flops=blocks * 2 * width * (2 * cap * width + 2 * cap * negatives + width * negatives),
            bytes_accessed=blocks * (cap * width + width * negatives) * 2,
            transcendentals=0,
        ),
    )(base, rows, slots, selves, wm, mb, ws, wn)


def score_kernel(parts, blocks, *refs):
    part_refs = refs[:parts]
    query_refs = refs[parts : parts + blocks]
    bias_ref, count_ref, embed_ref, peak_ref, total_ref = refs[parts + blocks :]
    hidden = bias_ref[...]
    for ref in part_refs:
        hidden = hidden + ref[...].astype(jnp.float32)
    hidden = jax.nn.relu(hidden)
    scale = lax.rsqrt(jnp.mean(hidden * hidden, axis=0, keepdims=True) + 0.25)
    embed_ref[...] = (hidden * scale).T.astype(jnp.bfloat16)
    log_count = jnp.log(count_ref[...].astype(jnp.float32))
    tile = 512
    for b in range(blocks):

        @pl.loop(0, query_refs[b].shape[0] // tile)
        def _(t):
            span = pl.ds(pl.multiple_of(t * tile, tile), tile)
            scores = (
                0.25
                * lax.dot_general(
                    embed_ref[...], query_refs[b][span, :], NT, preferred_element_type=jnp.float32
                )
                - log_count
            )
            peak = jnp.max(scores, axis=0, keepdims=True)
            peak_ref[b : b + 1, span] = peak
            total_ref[b : b + 1, span] = jnp.sum(jnp.exp(scores - peak), axis=0, keepdims=True)


def embed_and_score(parts, queries, bias, count):
    width, negatives = parts[0].shape
    rows = queries[0].shape[0]
    whole = pl.BlockSpec(memory_space=pltpu.VMEM)
    blocks = len(queries)
    return pl.pallas_call(
        functools.partial(score_kernel, len(parts), blocks),
        out_shape=(
            jax.ShapeDtypeStruct((negatives, width), jnp.bfloat16),
            jax.ShapeDtypeStruct((blocks, rows), jnp.float32),
            jax.ShapeDtypeStruct((blocks, rows), jnp.float32),
        ),
        in_specs=[whole] * (len(parts) + blocks + 2),
        out_specs=(whole,) * 3,
        cost_estimate=pl.CostEstimate(
            flops=2 * blocks * rows * negatives * width,
            bytes_accessed=2 * blocks * rows * width,
            transcendentals=blocks * rows * negatives,
        ),
    )(*parts, *queries, bias, count)


def swap(value, axis, offset):
    size = lax.axis_size(axis)
    if offset == 0:
        return value
    return lax.ppermute(value, axis, [(i, i ^ offset) for i in range(size)])


def per_device(
    items_table,
    fetch_rows,
    neighbour_slots,
    neighbour_count,
    self_slot,
    negative_count,
    message_weight,
    message_bias,
    self_weight,
    neighbour_weight,
    output_bias,
    queries,
):
    n_neg, n_qry = lax.axis_size("neg"), lax.axis_size("qry")
    own_neg, own_qry = lax.axis_index("neg"), lax.axis_index("qry")
    width = items_table.shape[1]
    cap = fetch_rows.shape[1]
    negatives, neighbours = neighbour_slots.shape
    groups = negatives // LANES

    live = jnp.arange(neighbours, dtype=jnp.int32)[None, :] < neighbour_count[:, None]
    slots = jnp.where(live, neighbour_slots, -1).T
    lists = jnp.concatenate([slots, self_slot[None, :]], axis=0).reshape(
        neighbours + 1, groups, LANES
    )
    far = list(range(n_neg - 1, -1, -1))
    wanted, asked = {}, {}
    for d in far:
        mine = lax.dynamic_index_in_dim(fetch_rows, own_neg ^ d, 0, keepdims=False)
        wanted[d] = swap(mine, "neg", d)
    for d in far:
        asked[d] = swap(lists, "neg", d)
    query_blocks = [swap(queries, "qry", d) for d in range(n_qry)]

    wm, ws, wn = message_weight.T, self_weight.T, neighbour_weight.T
    base = (own_neg * cap).astype(jnp.int32).reshape(1)
    per_call = 2
    parts = []
    for i in range(0, n_neg, per_call):
        offsets = far[i : i + per_call]
        index = jnp.concatenate([wanted[d] for d in offsets])
        rows = jnp.take(items_table, index, axis=0, mode="clip").reshape(
            len(offsets), cap, width
        )
        both = jnp.stack([asked[d] for d in offsets])
        part = partial_hidden(
            base, rows, both[:, :neighbours], both[:, neighbours], wm,
            message_bias[:, None], ws, wn,
        )
        for j, d in enumerate(offsets):
            parts.append(swap(part[j], "neg", d))

    count = lax.dynamic_slice_in_dim(negative_count, own_qry * negatives, negatives)
    negative_embed, peak, total = embed_and_score(
        parts, query_blocks, output_bias[:, None], count[:, None]
    )
    pairs = jnp.stack([peak, total], axis=1)
    pairs = jnp.stack([swap(pairs[d], "qry", d) for d in range(n_qry)])
    pairs = lax.all_gather(pairs, "neg").reshape(n_neg * n_qry, 2, -1)
    top = jnp.max(pairs[:, 0], axis=0)
    whole = jnp.sum(pairs[:, 1] * jnp.exp(pairs[:, 0] - top[None, :]), axis=0)
    query_lse = top + jnp.log(whole) - math.log(negatives * n_neg * n_qry)
    return (negative_embed, query_lse)


def solution(mesh):
    in_specs = (
        P("neg", None),
        P(("neg", "qry"), None),
        P(("neg", "qry"), None),
        P(("neg", "qry")),
        P(("neg", "qry")),
        P("neg"),
        P(),
        P(),
        P(),
        P(),
        P(),
        P("qry", None),
    )
    out_specs = (P(("neg", "qry"), None), P("qry"))
    return jax.shard_map(
        per_device, mesh=mesh, in_specs=in_specs, out_specs=out_specs, check_vma=False
    )
```

```python
import functools
import math

import jax
import jax.numpy as jnp
from jax import lax
from jax.experimental import pallas as pl
from jax.experimental.pallas import tpu as pltpu
from jax.sharding import PartitionSpec as P


LANES = 128
ROWS = 128
NT = (((1,), (1,)), ((), ()))


def sort_pairs(count):
    full = 1
    while full < count:
        full *= 2
    pairs = []
    p = 1
    while p < full:
        k = p
        while k >= 1:
            for j in range(k % p, full - k, 2 * k):
                for i in range(min(k, full - j - k)):
                    if (i + j) // (2 * p) == (i + j + k) // (2 * p):
                        if i + j + k < count:
                            pairs.append((i + j, i + j + k))
            k //= 2
        p *= 2
    return pairs


def gather_kernel(index_ref, table_ref, out_ref, wide_ref, picked_ref):
    block = pl.program_id(0)
    rows, width = table_ref.shape
    cap = out_ref.shape[1]
    pieces = width // LANES

    @pl.when(block == 0)
    def _():
        @pl.loop(0, rows // ROWS)
        def _(t):
            span = pl.ds(pl.multiple_of(t * ROWS, ROWS), ROWS)
            for c in range(pieces):
                wide_ref[pl.ds(t * ROWS * pieces + c, ROWS, stride=pieces), :] = table_ref[
                    span, c * LANES : (c + 1) * LANES
                ].astype(jnp.float32)

    unroll = 32

    @pl.loop(0, cap // unroll)
    def _(i):
        for u in range(unroll):
            place = i * unroll + u
            row = index_ref[block, place]
            picked_ref[pl.ds(pl.multiple_of(place * pieces, pieces), pieces), :] = wide_ref[
                pl.ds(pl.multiple_of(row * pieces, pieces), pieces), :
            ]

    @pl.loop(0, cap // ROWS)
    def _(t):
        span = pl.ds(pl.multiple_of(t * ROWS, ROWS), ROWS)
        for c in range(pieces):
            out_ref[0, span, c * LANES : (c + 1) * LANES] = picked_ref[
                pl.ds(t * ROWS * pieces + c, ROWS, stride=pieces), :
            ].astype(jnp.bfloat16)


def gather_rows(index, table):
    blocks, cap = index.shape
    rows, width = table.shape
    pieces = width // LANES
    return pl.pallas_call(
        gather_kernel,
        grid=(blocks,),
        out_shape=jax.ShapeDtypeStruct((blocks, cap, width), jnp.bfloat16),
        in_specs=[
            pl.BlockSpec(memory_space=pltpu.SMEM),
            pl.BlockSpec(memory_space=pltpu.VMEM),
        ],
        out_specs=pl.BlockSpec((1, cap, width), lambda b: (b, 0, 0)),
        scratch_shapes=[
            pltpu.VMEM((rows * pieces, LANES), jnp.float32),
            pltpu.VMEM((cap * pieces, LANES), jnp.float32),
        ],
        compiler_params=pltpu.CompilerParams(vmem_limit_bytes=48 << 20),
        cost_estimate=pl.CostEstimate(
            flops=0, bytes_accessed=(rows + blocks * cap) * width * 2 * 4, transcendentals=0
        ),
    )(index, table)


def partial_kernel(
    base_ref, rows_ref, slots_ref, wm_ref, mb_ref, ws_ref, wn_ref,
    out_ref, order_ref, times_ref, counts_ref, self_hot_ref,
):
    cap = rows_ref.shape[1]
    neighbours, groups = slots_ref.shape[0] - 1, slots_ref.shape[1]
    packed = 16
    chunk = 320 if cap % 320 == 0 else ROWS
    big = jnp.int32(32767)
    base = base_ref[0]
    places = []
    live = jnp.zeros((groups, LANES), jnp.int32)
    mine = jnp.zeros((groups, LANES), jnp.int32)
    for k in range(neighbours):
        slot = slots_ref[k]
        local = slot - base
        inside = (local >= 0) & (local < cap) & (slot >= 0)
        live = live + jnp.where(slot >= 0, 1, 0)
        mine = mine + jnp.where(inside, 1, 0)
        places.append(jnp.where(inside, local, big))
    for a, b in sort_pairs(neighbours):
        low, high = jnp.minimum(places[a], places[b]), jnp.maximum(places[a], places[b])
        places[a], places[b] = low, high
    run = jnp.ones((groups, LANES), jnp.float32)
    for k in range(neighbours):
        if k:
            run = jnp.where(places[k] == places[k - 1], run + 1.0, 1.0)
        for g in range(groups):
            tile = (packed, LANES)
            order_ref[g, k] = jnp.broadcast_to(places[k][g : g + 1], tile).astype(jnp.int16)
            times_ref[g, k] = jnp.broadcast_to(run[g : g + 1], tile).astype(jnp.bfloat16)
    inverse = 1.0 / live.astype(jnp.float32)
    own = slots_ref[neighbours] - base
    own = jnp.where((own >= 0) & (own < cap), own, big)
    iota = lax.broadcasted_iota(jnp.int32, (packed, LANES), 0)
    tiles = chunk // packed
    unroll = 4
    for g in range(groups):
        lanes = pl.ds(g * LANES, LANES)
        steps = (jnp.max(mine[g : g + 1]) + unroll - 1) // unroll
        own_tile = jnp.broadcast_to(own[g : g + 1], (packed, LANES)).astype(jnp.int16)

        @pl.loop(0, cap // chunk)
        def _(c):
            first = c * chunk
            here = [(iota + (first + packed * i)).astype(jnp.int16) for i in range(tiles)]

            def step(i, totals):
                for u in range(unroll):
                    k = unroll * i + u
                    slot, times = order_ref[g, k], times_ref[g, k]
                    totals = tuple(
                        jnp.where(here[j] == slot, times, totals[j]) for j in range(tiles)
                    )
                return totals

            zero = jnp.zeros((packed, LANES), jnp.bfloat16)
            one = jnp.ones((packed, LANES), jnp.bfloat16)
            totals = lax.fori_loop(0, steps, step, (zero,) * tiles)
            for j in range(tiles):
                span = pl.ds(pl.multiple_of(first + packed * j, packed), packed)
                counts_ref[span, lanes] = totals[j]
                self_hot_ref[span, lanes] = jnp.where(here[j] == own_tile, one, zero)

    rows = rows_ref[0]
    message = jax.nn.relu(
        lax.dot_general(wm_ref[...], rows, NT, preferred_element_type=jnp.float32) + mb_ref[...]
    ).astype(jnp.bfloat16)
    summed = jnp.dot(message, counts_ref[...], preferred_element_type=jnp.float32)
    scale = jnp.concatenate([inverse[g : g + 1, :] for g in range(groups)], axis=1)
    mean = (summed * scale).astype(jnp.bfloat16)
    own_part = lax.dot_general(ws_ref[...], rows, NT, preferred_element_type=jnp.float32).astype(
        jnp.bfloat16
    )
    part = jnp.dot(own_part, self_hot_ref[...], preferred_element_type=jnp.float32)
    part = part + jnp.dot(wn_ref[...], mean, preferred_element_type=jnp.float32)
    out_ref[...] = part.astype(jnp.bfloat16)


def partial_hidden(base, rows, which, lists, wm, mb, ws, wn):
    _, cap, width = rows.shape
    neighbours, groups = lists.shape[0] - 1, lists.shape[1]
    negatives = groups * LANES
    whole = pl.BlockSpec(memory_space=pltpu.VMEM)
    return pl.pallas_call(
        partial_kernel,
        grid=(1,),
        out_shape=jax.ShapeDtypeStruct((width, negatives), jnp.bfloat16),
        in_specs=[
            pl.BlockSpec(memory_space=pltpu.SMEM),
            pl.BlockSpec((1, cap, width), lambda b: (which, 0, 0)),
            whole, whole, whole, whole, whole,
        ],
        out_specs=pl.BlockSpec((width, negatives), lambda b: (0, 0)),
        scratch_shapes=[
            pltpu.VMEM((groups, neighbours, 16, LANES), jnp.int16),
            pltpu.VMEM((groups, neighbours, 16, LANES), jnp.bfloat16),
            pltpu.VMEM((cap, negatives), jnp.bfloat16),
            pltpu.VMEM((cap, negatives), jnp.bfloat16),
        ],
        cost_estimate=pl.CostEstimate(
            flops=2 * width * (2 * cap * width + 2 * cap * negatives + width * negatives) * 2,
            bytes_accessed=(cap * width + width * negatives) * 2,
            transcendentals=0,
        ),
    )(base, rows, lists, wm, mb, ws, wn)


def score_kernel(parts, blocks, *refs):
    part_refs = refs[:parts]
    query_refs = refs[parts : parts + blocks]
    bias_ref, count_ref, embed_ref, peak_ref, total_ref = refs[parts + blocks :]
    hidden = bias_ref[...]
    for ref in part_refs:
        hidden = hidden + ref[...].astype(jnp.float32)
    hidden = jax.nn.relu(hidden)
    scale = lax.rsqrt(jnp.mean(hidden * hidden, axis=0, keepdims=True) + 0.25)
    embed_ref[...] = (hidden * scale).T.astype(jnp.bfloat16)
    log_count = jnp.log(count_ref[...].astype(jnp.float32))
    tile = 512
    for b in range(blocks):

        @pl.loop(0, query_refs[b].shape[0] // tile)
        def _(t):
            span = pl.ds(pl.multiple_of(t * tile, tile), tile)
            scores = (
                0.25
                * lax.dot_general(
                    embed_ref[...], query_refs[b][span, :], NT, preferred_element_type=jnp.float32
                )
                - log_count
            )
            peak = jnp.max(scores, axis=0, keepdims=True)
            peak_ref[b : b + 1, span] = peak
            total_ref[b : b + 1, span] = jnp.sum(jnp.exp(scores - peak), axis=0, keepdims=True)


def embed_and_score(parts, queries, bias, count):
    width, negatives = parts[0].shape
    rows = queries[0].shape[0]
    whole = pl.BlockSpec(memory_space=pltpu.VMEM)
    blocks = len(queries)
    return pl.pallas_call(
        functools.partial(score_kernel, len(parts), blocks),
        out_shape=(
            jax.ShapeDtypeStruct((negatives, width), jnp.bfloat16),
            jax.ShapeDtypeStruct((blocks, rows), jnp.float32),
            jax.ShapeDtypeStruct((blocks, rows), jnp.float32),
        ),
        in_specs=[whole] * (len(parts) + blocks + 2),
        out_specs=(whole,) * 3,
        cost_estimate=pl.CostEstimate(
            flops=2 * blocks * rows * negatives * width,
            bytes_accessed=2 * blocks * rows * width,
            transcendentals=blocks * rows * negatives,
        ),
    )(*parts, *queries, bias, count)


def swap(value, axis, offset):
    size = lax.axis_size(axis)
    if offset == 0:
        return value
    return lax.ppermute(value, axis, [(i, i ^ offset) for i in range(size)])


def per_device(
    items_table,
    fetch_rows,
    neighbour_slots,
    neighbour_count,
    self_slot,
    negative_count,
    message_weight,
    message_bias,
    self_weight,
    neighbour_weight,
    output_bias,
    queries,
):
    n_neg, n_qry = lax.axis_size("neg"), lax.axis_size("qry")
    own_neg, own_qry = lax.axis_index("neg"), lax.axis_index("qry")
    width = items_table.shape[1]
    cap = fetch_rows.shape[1]
    negatives, neighbours = neighbour_slots.shape
    groups = negatives // LANES

    live = jnp.arange(neighbours, dtype=jnp.int32)[None, :] < neighbour_count[:, None]
    slots = jnp.where(live, neighbour_slots, -1).T
    lists = jnp.concatenate([slots, self_slot[None, :]], axis=0).reshape(
        neighbours + 1, groups, LANES
    )
    far = sorted(range(n_neg), key=lambda d: (-(d // 2).bit_count(), -d))
    wanted, asked = {}, {}
    for d in far:
        mine = lax.dynamic_index_in_dim(fetch_rows, own_neg ^ d, 0, keepdims=False)
        wanted[d] = swap(mine, "neg", d)
    for d in far:
        asked[d] = swap(lists, "neg", d)
    query_blocks = [swap(queries, "qry", d) for d in range(n_qry)]

    wm, ws, wn = message_weight.T, self_weight.T, neighbour_weight.T
    base = (own_neg * cap).astype(jnp.int32).reshape(1)
    rows = gather_rows(jnp.stack([wanted[d] for d in far]), items_table)
    parts = []
    for j, d in enumerate(far):
        part = partial_hidden(
            base, rows, j, asked[d], wm, message_bias[:, None], ws, wn
        )
        base, part = lax.optimization_barrier((base, part))
        parts.append(swap(part, "neg", d))

    count = lax.dynamic_slice_in_dim(negative_count, own_qry * negatives, negatives)
    negative_embed, peak, total = embed_and_score(
        parts, query_blocks, output_bias[:, None], count[:, None]
    )
    pairs = jnp.stack([peak, total], axis=1)
    pairs = jnp.stack([swap(pairs[d], "qry", d) for d in range(n_qry)])
    pairs = lax.all_gather(pairs, "neg").reshape(n_neg * n_qry, 2, -1)
    top = jnp.max(pairs[:, 0], axis=0)
    whole = jnp.sum(pairs[:, 1] * jnp.exp(pairs[:, 0] - top[None, :]), axis=0)
    query_lse = top + jnp.log(whole) - math.log(negatives * n_neg * n_qry)
    return (negative_embed, query_lse)


def solution(mesh):
    in_specs = (
        P("neg", None),
        P(("neg", "qry"), None),
        P(("neg", "qry"), None),
        P(("neg", "qry")),
        P(("neg", "qry")),
        P("neg"),
        P(),
        P(),
        P(),
        P(),
        P(),
        P("qry", None),
    )
    out_specs = (P(("neg", "qry"), None), P("qry"))
    return jax.shard_map(
        per_device, mesh=mesh, in_specs=in_specs, out_specs=out_specs, check_vma=False
    )
```

```python
import functools
import math

import jax
import jax.numpy as jnp
from jax import lax
from jax.experimental import pallas as pl
from jax.experimental.pallas import tpu as pltpu
from jax.sharding import PartitionSpec as P


LANES = 128
ROWS = 128
DEAD = 32767
NT = (((1,), (1,)), ((), ()))


def sort_pairs(count):
    full = 1
    while full < count:
        full *= 2
    pairs = []
    p = 1
    while p < full:
        k = p
        while k >= 1:
            for j in range(k % p, full - k, 2 * k):
                for i in range(min(k, full - j - k)):
                    if (i + j) // (2 * p) == (i + j + k) // (2 * p):
                        if i + j + k < count:
                            pairs.append((i + j, i + j + k))
            k //= 2
        p *= 2
    return pairs


def gather_kernel(index_ref, table_ref, *refs):
    weights, out_ref, flipped, (wide_ref, picked_ref) = refs[:3], refs[3], refs[4:7], refs[7:]
    block = pl.program_id(0)
    rows, width = table_ref.shape
    cap = out_ref.shape[1]
    pieces = width // LANES

    @pl.when(block == 0)
    def _():
        for weight, turned in zip(weights, flipped):
            turned[...] = weight[...].T

        @pl.loop(0, rows // ROWS)
        def _(t):
            span = pl.ds(pl.multiple_of(t * ROWS, ROWS), ROWS)
            for c in range(pieces):
                wide_ref[pl.ds(t * ROWS * pieces + c, ROWS, stride=pieces), :] = table_ref[
                    span, c * LANES : (c + 1) * LANES
                ].astype(jnp.float32)

    unroll = 32

    @pl.loop(0, cap // unroll)
    def _(i):
        for u in range(unroll):
            place = i * unroll + u
            row = pl.multiple_of(index_ref[block, place], pieces)
            picked_ref[pl.ds(pl.multiple_of(place * pieces, pieces), pieces), :] = wide_ref[
                pl.ds(row, pieces), :
            ]

    @pl.loop(0, cap // ROWS)
    def _(t):
        span = pl.ds(pl.multiple_of(t * ROWS, ROWS), ROWS)
        for c in range(pieces):
            out_ref[0, span, c * LANES : (c + 1) * LANES] = picked_ref[
                pl.ds(t * ROWS * pieces + c, ROWS, stride=pieces), :
            ].astype(jnp.bfloat16)


def gather_rows(index, table, weights):
    blocks, cap = index.shape
    rows, width = table.shape
    pieces = width // LANES
    return pl.pallas_call(
        gather_kernel,
        grid=(blocks,),
        out_shape=[jax.ShapeDtypeStruct((blocks, cap, width), jnp.bfloat16)]
        + [jax.ShapeDtypeStruct(w.shape[::-1], w.dtype) for w in weights],
        in_specs=[pl.BlockSpec(memory_space=pltpu.SMEM)]
        + [pl.BlockSpec(memory_space=pltpu.VMEM)] * 4,
        out_specs=[pl.BlockSpec((1, cap, width), lambda b: (b, 0, 0))]
        + [pl.BlockSpec(memory_space=pltpu.VMEM)] * 3,
        scratch_shapes=[
            pltpu.VMEM((rows * pieces, LANES), jnp.float32),
            pltpu.VMEM((cap * pieces, LANES), jnp.float32),
        ],
        compiler_params=pltpu.CompilerParams(vmem_limit_bytes=48 << 20),
    )(index * pieces, table, *weights)


def partial_kernel(
    base_ref, rows_ref, slots_ref, wm_ref, mb_ref, ws_ref, wn_ref,
    out_ref, order_ref, times_ref, counts_ref, self_hot_ref,
):
    cap = rows_ref.shape[1]
    negatives = counts_ref.shape[1]
    groups, neighbours = negatives // LANES, times_ref.shape[1]
    half = neighbours // 2
    packed = 16
    chunk = 320 if cap % 320 == 0 else ROWS
    big = jnp.int32(32767)
    base = base_ref[0]
    places = []
    live = jnp.zeros((groups, LANES), jnp.int32)
    mine = jnp.zeros((groups, LANES), jnp.int32)
    for k in range(neighbours):
        word = slots_ref[(k % half) * groups : (k % half + 1) * groups, :]
        slot = word & DEAD if k < half else word >> 16
        local = slot - base
        inside = (local >= 0) & (local < cap)
        live = live + jnp.where(slot < DEAD, 1, 0)
        mine = mine + jnp.where(inside, 1, 0)
        places.append(jnp.where(inside, local, big))
    for a, b in sort_pairs(neighbours):
        low, high = jnp.minimum(places[a], places[b]), jnp.maximum(places[a], places[b])
        places[a], places[b] = low, high
    run = jnp.ones((groups, LANES), jnp.float32)
    for k in range(neighbours):
        if k:
            run = jnp.where(places[k] == places[k - 1], run + 1.0, 1.0)
        for g in range(groups):
            tile = (packed, LANES)
            order_ref[g, k] = jnp.broadcast_to(places[k][g : g + 1], tile).astype(jnp.int16)
            times_ref[g, k] = jnp.broadcast_to(run[g : g + 1], tile).astype(jnp.bfloat16)
    inverse = 1.0 / live.astype(jnp.float32)
    own = slots_ref[half * groups : (half + 1) * groups, :] - base
    own = jnp.where((own >= 0) & (own < cap), own, big)
    iota = lax.broadcasted_iota(jnp.int32, (packed, LANES), 0)
    tiles = chunk // packed
    unroll = 4
    for g in range(groups):
        lanes = pl.ds(g * LANES, LANES)
        steps = (jnp.max(mine[g : g + 1]) + unroll - 1) // unroll
        own_tile = jnp.broadcast_to(own[g : g + 1], (packed, LANES)).astype(jnp.int16)

        @pl.loop(0, cap // chunk)
        def _(c):
            first = c * chunk
            here = [(iota + (first + packed * i)).astype(jnp.int16) for i in range(tiles)]

            def step(i, totals):
                for u in range(unroll):
                    k = unroll * i + u
                    slot, times = order_ref[g, k], times_ref[g, k]
                    totals = tuple(
                        jnp.where(here[j] == slot, times, totals[j]) for j in range(tiles)
                    )
                return totals

            zero = jnp.zeros((packed, LANES), jnp.bfloat16)
            one = jnp.ones((packed, LANES), jnp.bfloat16)
            totals = lax.fori_loop(0, steps, step, (zero,) * tiles)
            for j in range(tiles):
                span = pl.ds(pl.multiple_of(first + packed * j, packed), packed)
                counts_ref[span, lanes] = totals[j]
                self_hot_ref[span, lanes] = jnp.where(here[j] == own_tile, one, zero)

    rows = rows_ref[0]
    message = jax.nn.relu(
        lax.dot_general(wm_ref[...], rows, NT, preferred_element_type=jnp.float32) + mb_ref[...]
    ).astype(jnp.bfloat16)
    summed = jnp.dot(message, counts_ref[...], preferred_element_type=jnp.float32)
    scale = jnp.concatenate([inverse[g : g + 1, :] for g in range(groups)], axis=1)
    mean = (summed * scale).astype(jnp.bfloat16)
    own_part = lax.dot_general(ws_ref[...], rows, NT, preferred_element_type=jnp.float32).astype(
        jnp.bfloat16
    )
    part = jnp.dot(own_part, self_hot_ref[...], preferred_element_type=jnp.float32)
    part = part + jnp.dot(wn_ref[...], mean, preferred_element_type=jnp.float32)
    out_ref[...] = part.astype(jnp.bfloat16)


def partial_hidden(base, rows, which, lists, shape, wm, mb, ws, wn):
    _, cap, width = rows.shape
    negatives, neighbours = shape
    groups = negatives // LANES
    whole = pl.BlockSpec(memory_space=pltpu.VMEM)
    return pl.pallas_call(
        partial_kernel,
        grid=(1,),
        out_shape=jax.ShapeDtypeStruct((width, negatives), jnp.bfloat16),
        in_specs=[
            pl.BlockSpec(memory_space=pltpu.SMEM),
            pl.BlockSpec((1, cap, width), lambda b: (which, 0, 0)),
            whole, whole, whole, whole, whole,
        ],
        out_specs=pl.BlockSpec((width, negatives), lambda b: (0, 0)),
        scratch_shapes=[
            pltpu.VMEM((groups, neighbours, 16, LANES), jnp.int16),
            pltpu.VMEM((groups, neighbours, 16, LANES), jnp.bfloat16),
            pltpu.VMEM((cap, negatives), jnp.bfloat16),
            pltpu.VMEM((cap, negatives), jnp.bfloat16),
        ],
    )(base, rows, lists, wm, mb, ws, wn)


def score_kernel(parts, blocks, *refs):
    part_refs = refs[:parts]
    query_refs = refs[parts : parts + blocks]
    bias_ref, count_ref, embed_ref, peak_ref, total_ref = refs[parts + blocks :]
    hidden = bias_ref[...]
    for ref in part_refs:
        hidden = hidden + ref[...].astype(jnp.float32)
    hidden = jax.nn.relu(hidden)
    scale = lax.rsqrt(jnp.mean(hidden * hidden, axis=0, keepdims=True) + 0.25)
    embed_ref[...] = (hidden * scale).T.astype(jnp.bfloat16)
    log_count = jnp.log(count_ref[...].astype(jnp.float32))
    tile = 512
    for b in range(blocks):

        @pl.loop(0, query_refs[b].shape[0] // tile)
        def _(t):
            span = pl.ds(pl.multiple_of(t * tile, tile), tile)
            scores = (
                0.25
                * lax.dot_general(
                    embed_ref[...], query_refs[b][span, :], NT, preferred_element_type=jnp.float32
                )
                - log_count
            )
            peak = jnp.max(scores, axis=0, keepdims=True)
            peak_ref[b : b + 1, span] = peak
            total_ref[b : b + 1, span] = jnp.sum(jnp.exp(scores - peak), axis=0, keepdims=True)


def embed_and_score(parts, queries, bias, count):
    width, negatives = parts[0].shape
    rows = queries[0].shape[0]
    whole = pl.BlockSpec(memory_space=pltpu.VMEM)
    blocks = len(queries)
    return pl.pallas_call(
        functools.partial(score_kernel, len(parts), blocks),
        out_shape=(
            jax.ShapeDtypeStruct((negatives, width), jnp.bfloat16),
            jax.ShapeDtypeStruct((blocks, rows), jnp.float32),
            jax.ShapeDtypeStruct((blocks, rows), jnp.float32),
        ),
        in_specs=[whole] * (len(parts) + blocks + 2),
        out_specs=(whole,) * 3,
        cost_estimate=pl.CostEstimate(
            flops=2 * blocks * rows * negatives * width,
            bytes_accessed=2 * blocks * rows * width,
            transcendentals=blocks * rows * negatives,
        ),
    )(*parts, *queries, bias, count)


def swap(value, axis, offset):
    size = lax.axis_size(axis)
    if offset == 0:
        return value
    return lax.ppermute(value, axis, [(i, i ^ offset) for i in range(size)])


def per_device(
    items_table,
    fetch_rows,
    neighbour_slots,
    neighbour_count,
    self_slot,
    negative_count,
    message_weight,
    message_bias,
    self_weight,
    neighbour_weight,
    output_bias,
    queries,
):
    n_neg, n_qry = lax.axis_size("neg"), lax.axis_size("qry")
    own_neg, own_qry = lax.axis_index("neg"), lax.axis_index("qry")
    cap = fetch_rows.shape[1]
    negatives, neighbours = neighbour_slots.shape
    groups = negatives // LANES

    assert n_neg * cap < DEAD and neighbours % 4 == 0
    live = jnp.arange(neighbours, dtype=jnp.int32)[None, :] < neighbour_count[:, None]
    slots = jnp.where(live, neighbour_slots, DEAD).T
    half = neighbours // 2
    words = slots[:half] | (slots[half:] << 16)
    lists = jnp.concatenate([words.reshape(-1, LANES), self_slot.reshape(-1, LANES)])
    far = sorted(range(n_neg), key=lambda d: (-(d // 2).bit_count(), -(d % 2), -d))
    asked = {}
    for d in far:
        mine = lax.dynamic_index_in_dim(fetch_rows, own_neg ^ d, 0, keepdims=False)
        asked[d] = swap(jnp.concatenate([lists, mine.reshape(-1, LANES)]), "neg", d)
    query_blocks = [queries]
    for d in range(1, n_qry):
        query_blocks.append(swap(queries, "qry", d))

    base = (own_neg * cap).astype(jnp.int32).reshape(1)
    wanted = jnp.stack([asked[d][(half + 1) * groups :].reshape(cap) for d in far])
    rows, wm, ws, wn = gather_rows(
        wanted, items_table, (message_weight, self_weight, neighbour_weight)
    )
    parts = []
    for j, d in enumerate(far):
        part = partial_hidden(
            base, rows, j, asked[d], (negatives, neighbours), wm, message_bias[:, None], ws, wn
        )
        base, part = lax.optimization_barrier((base, part))
        parts.append(swap(part, "neg", d))

    count = lax.dynamic_slice_in_dim(negative_count, own_qry * negatives, negatives)
    negative_embed, peak, total = embed_and_score(
        parts, query_blocks, output_bias[:, None], count[:, None]
    )
    pairs = jnp.stack([peak, total], axis=1)
    pairs = jnp.stack([swap(pairs[d], "qry", d) for d in range(n_qry)])
    pairs = lax.all_gather(pairs, "neg").reshape(n_neg * n_qry, 2, -1)
    top = jnp.max(pairs[:, 0], axis=0)
    whole = jnp.sum(pairs[:, 1] * jnp.exp(pairs[:, 0] - top[None, :]), axis=0)
    query_lse = top + jnp.log(whole) - math.log(negatives * n_neg * n_qry)
    return (negative_embed, query_lse)


def solution(mesh):
    in_specs = (
        P("neg", None),
        P(("neg", "qry"), None),
        P(("neg", "qry"), None),
        P(("neg", "qry")),
        P(("neg", "qry")),
        P("neg"),
        P(),
        P(),
        P(),
        P(),
        P(),
        P("qry", None),
    )
    out_specs = (P(("neg", "qry"), None), P("qry"))
    return jax.shard_map(
        per_device, mesh=mesh, in_specs=in_specs, out_specs=out_specs, check_vma=False
    )
```

```python
import functools
import math

import jax
import jax.numpy as jnp
from jax import lax
from jax.experimental import pallas as pl
from jax.experimental.pallas import tpu as pltpu
from jax.sharding import PartitionSpec as P


LANES = 128
ROWS = 128
DEAD = 32767
NT = (((1,), (1,)), ((), ()))


def sort_pairs(count):
    full = 1
    while full < count:
        full *= 2
    pairs = []
    p = 1
    while p < full:
        k = p
        while k >= 1:
            for j in range(k % p, full - k, 2 * k):
                for i in range(min(k, full - j - k)):
                    if (i + j) // (2 * p) == (i + j + k) // (2 * p):
                        if i + j + k < count:
                            pairs.append((i + j, i + j + k))
            k //= 2
        p *= 2
    return pairs


def gather_kernel(index_ref, table_ref, *refs):
    weights, out_ref, flipped, (wide_ref, picked_ref) = refs[:3], refs[3], refs[4:7], refs[7:]
    block = pl.program_id(0)
    rows, width = table_ref.shape
    cap = out_ref.shape[1]
    pieces = width // LANES

    @pl.when(block == 0)
    def _():
        for weight, turned in zip(weights, flipped):
            turned[...] = weight[...].T

        @pl.loop(0, rows // ROWS)
        def _(t):
            span = pl.ds(pl.multiple_of(t * ROWS, ROWS), ROWS)
            for c in range(pieces):
                wide_ref[pl.ds(t * ROWS * pieces + c, ROWS, stride=pieces), :] = table_ref[
                    span, c * LANES : (c + 1) * LANES
                ].astype(jnp.float32)

    unroll = 32

    @pl.loop(0, cap // unroll)
    def _(i):
        first = block * cap + i * unroll
        start = pl.multiple_of(i * (unroll * pieces), unroll * pieces)
        places = [pl.multiple_of(index_ref[first + u], pieces) for u in range(unroll)]
        for u in range(unroll):
            picked_ref[pl.ds(start + u * pieces, pieces), :] = wide_ref[
                pl.ds(places[u], pieces), :
            ]

    @pl.loop(0, cap // ROWS)
    def _(t):
        span = pl.ds(pl.multiple_of(t * ROWS, ROWS), ROWS)
        for c in range(pieces):
            out_ref[0, span, c * LANES : (c + 1) * LANES] = picked_ref[
                pl.ds(t * ROWS * pieces + c, ROWS, stride=pieces), :
            ].astype(jnp.bfloat16)


def gather_rows(index, cap, table, weights):
    blocks = index.shape[0] // cap
    rows, width = table.shape
    pieces = width // LANES
    return pl.pallas_call(
        gather_kernel,
        grid=(blocks,),
        out_shape=[jax.ShapeDtypeStruct((blocks, cap, width), jnp.bfloat16)]
        + [jax.ShapeDtypeStruct(w.shape[::-1], w.dtype) for w in weights],
        in_specs=[pl.BlockSpec(memory_space=pltpu.SMEM)]
        + [pl.BlockSpec(memory_space=pltpu.VMEM)] * 4,
        out_specs=[pl.BlockSpec((1, cap, width), lambda b: (b, 0, 0))]
        + [pl.BlockSpec(memory_space=pltpu.VMEM)] * 3,
        scratch_shapes=[
            pltpu.VMEM((rows * pieces, LANES), jnp.float32),
            pltpu.VMEM((cap * pieces, LANES), jnp.float32),
        ],
        compiler_params=pltpu.CompilerParams(vmem_limit_bytes=48 << 20),
    )(index * pieces, table, *weights)


def partial_kernel(
    base_ref, rows_ref, slots_ref, wm_ref, mb_ref, ws_ref, wn_ref,
    out_ref, order_ref, times_ref, counts_ref, self_hot_ref,
):
    cap = rows_ref.shape[1]
    negatives = counts_ref.shape[1]
    groups, neighbours = negatives // LANES, times_ref.shape[1]
    half = neighbours // 2
    packed = 16
    chunk = 320 if cap % 320 == 0 else ROWS
    big = jnp.int32(32767)
    base = base_ref[0]
    places = []
    live = jnp.zeros((groups, LANES), jnp.int32)
    mine = jnp.zeros((groups, LANES), jnp.int32)
    for k in range(neighbours):
        word = slots_ref[(k % half) * groups : (k % half + 1) * groups, :]
        slot = word & DEAD if k < half else word >> 16
        local = slot - base
        inside = (local >= 0) & (local < cap)
        live = live + jnp.where(slot < DEAD, 1, 0)
        mine = mine + jnp.where(inside, 1, 0)
        places.append(jnp.where(inside, local, big))
    for a, b in sort_pairs(neighbours):
        low, high = jnp.minimum(places[a], places[b]), jnp.maximum(places[a], places[b])
        places[a], places[b] = low, high
    run = jnp.ones((groups, LANES), jnp.float32)
    for k in range(neighbours):
        if k:
            run = jnp.where(places[k] == places[k - 1], run + 1.0, 1.0)
        for g in range(groups):
            tile = (packed, LANES)
            order_ref[g, k] = jnp.broadcast_to(places[k][g : g + 1], tile).astype(jnp.int16)
            times_ref[g, k] = jnp.broadcast_to(run[g : g + 1], tile).astype(jnp.bfloat16)
    inverse = 1.0 / live.astype(jnp.float32)
    own = slots_ref[half * groups : (half + 1) * groups, :] - base
    own = jnp.where((own >= 0) & (own < cap), own, big)
    iota = lax.broadcasted_iota(jnp.int32, (packed, LANES), 0)
    tiles = chunk // packed
    unroll = 4
    for g in range(groups):
        lanes = pl.ds(g * LANES, LANES)
        steps = (jnp.max(mine[g : g + 1]) + unroll - 1) // unroll
        own_tile = jnp.broadcast_to(own[g : g + 1], (packed, LANES)).astype(jnp.int16)

        @pl.loop(0, cap // chunk)
        def _(c):
            first = c * chunk
            here = [(iota + (first + packed * i)).astype(jnp.int16) for i in range(tiles)]

            def step(i, totals):
                for u in range(unroll):
                    k = unroll * i + u
                    slot, times = order_ref[g, k], times_ref[g, k]
                    totals = tuple(
                        jnp.where(here[j] == slot, times, totals[j]) for j in range(tiles)
                    )
                return totals

            zero = jnp.zeros((packed, LANES), jnp.bfloat16)
            one = jnp.ones((packed, LANES), jnp.bfloat16)
            totals = lax.fori_loop(0, steps, step, (zero,) * tiles)
            for j in range(tiles):
                span = pl.ds(pl.multiple_of(first + packed * j, packed), packed)
                counts_ref[span, lanes] = totals[j]
                self_hot_ref[span, lanes] = jnp.where(here[j] == own_tile, one, zero)

    rows = rows_ref[0]
    message = jax.nn.relu(
        lax.dot_general(wm_ref[...], rows, NT, preferred_element_type=jnp.float32) + mb_ref[...]
    ).astype(jnp.bfloat16)
    summed = jnp.dot(message, counts_ref[...], preferred_element_type=jnp.float32)
    scale = jnp.concatenate([inverse[g : g + 1, :] for g in range(groups)], axis=1)
    mean = (summed * scale).astype(jnp.bfloat16)
    own_part = lax.dot_general(ws_ref[...], rows, NT, preferred_element_type=jnp.float32).astype(
        jnp.bfloat16
    )
    part = jnp.dot(own_part, self_hot_ref[...], preferred_element_type=jnp.float32)
    part = part + jnp.dot(wn_ref[...], mean, preferred_element_type=jnp.float32)
    out_ref[...] = part.astype(jnp.bfloat16)


def partial_hidden(base, rows, which, lists, shape, wm, mb, ws, wn):
    _, cap, width = rows.shape
    negatives, neighbours = shape
    groups = negatives // LANES
    whole = pl.BlockSpec(memory_space=pltpu.VMEM)
    return pl.pallas_call(
        partial_kernel,
        grid=(1,),
        out_shape=jax.ShapeDtypeStruct((width, negatives), jnp.bfloat16),
        in_specs=[
            pl.BlockSpec(memory_space=pltpu.SMEM),
            pl.BlockSpec((1, cap, width), lambda b: (which, 0, 0)),
            whole, whole, whole, whole, whole,
        ],
        out_specs=pl.BlockSpec((width, negatives), lambda b: (0, 0)),
        scratch_shapes=[
            pltpu.VMEM((groups, neighbours, 16, LANES), jnp.int16),
            pltpu.VMEM((groups, neighbours, 16, LANES), jnp.bfloat16),
            pltpu.VMEM((cap, negatives), jnp.bfloat16),
            pltpu.VMEM((cap, negatives), jnp.bfloat16),
        ],
    )(base, rows, lists, wm, mb, ws, wn)


def score_kernel(parts, blocks, *refs):
    part_refs = refs[:parts]
    query_refs = refs[parts : parts + blocks]
    bias_ref, count_ref, embed_ref, peak_ref, total_ref = refs[parts + blocks :]
    hidden = bias_ref[...]
    for ref in part_refs:
        hidden = hidden + ref[...].astype(jnp.float32)
    hidden = jax.nn.relu(hidden)
    scale = lax.rsqrt(jnp.mean(hidden * hidden, axis=0, keepdims=True) + 0.25)
    embed_ref[...] = (hidden * scale).T.astype(jnp.bfloat16)
    log_count = jnp.log(count_ref[...].astype(jnp.float32))
    tile = 512
    for b in range(blocks):

        @pl.loop(0, query_refs[b].shape[0] // tile)
        def _(t):
            span = pl.ds(pl.multiple_of(t * tile, tile), tile)
            scores = (
                0.25
                * lax.dot_general(
                    embed_ref[...], query_refs[b][span, :], NT, preferred_element_type=jnp.float32
                )
                - log_count
            )
            peak = jnp.max(scores, axis=0, keepdims=True)
            peak_ref[b : b + 1, span] = peak
            total_ref[b : b + 1, span] = jnp.sum(jnp.exp(scores - peak), axis=0, keepdims=True)


def embed_and_score(parts, queries, bias, count):
    width, negatives = parts[0].shape
    rows = queries[0].shape[0]
    whole = pl.BlockSpec(memory_space=pltpu.VMEM)
    blocks = len(queries)
    return pl.pallas_call(
        functools.partial(score_kernel, len(parts), blocks),
        out_shape=(
            jax.ShapeDtypeStruct((negatives, width), jnp.bfloat16),
            jax.ShapeDtypeStruct((blocks, rows), jnp.float32),
            jax.ShapeDtypeStruct((blocks, rows), jnp.float32),
        ),
        in_specs=[whole] * (len(parts) + blocks + 2),
        out_specs=(whole,) * 3,
        cost_estimate=pl.CostEstimate(
            flops=2 * blocks * rows * negatives * width,
            bytes_accessed=2 * blocks * rows * width,
            transcendentals=blocks * rows * negatives,
        ),
    )(*parts, *queries, bias, count)


def swap(value, axis, offset):
    size = lax.axis_size(axis)
    if offset == 0:
        return value
    return lax.ppermute(value, axis, [(i, i ^ offset) for i in range(size)])


def per_device(
    items_table,
    fetch_rows,
    neighbour_slots,
    neighbour_count,
    self_slot,
    negative_count,
    message_weight,
    message_bias,
    self_weight,
    neighbour_weight,
    output_bias,
    queries,
):
    n_neg, n_qry = lax.axis_size("neg"), lax.axis_size("qry")
    own_neg, own_qry = lax.axis_index("neg"), lax.axis_index("qry")
    cap = fetch_rows.shape[1]
    negatives, neighbours = neighbour_slots.shape
    groups = negatives // LANES

    assert n_neg * cap < DEAD and neighbours % 4 == 0
    live = jnp.arange(neighbours, dtype=jnp.int32)[None, :] < neighbour_count[:, None]
    slots = jnp.where(live, neighbour_slots, DEAD).T
    half = neighbours // 2
    words = slots[:half] | (slots[half:] << 16)
    lists = jnp.concatenate([words.reshape(-1, LANES), self_slot.reshape(-1, LANES)])
    far = sorted(range(n_neg), key=lambda d: (-(d // 2).bit_count(), -(d % 2), -d))
    asked = {}
    for d in far:
        mine = lax.dynamic_index_in_dim(fetch_rows, own_neg ^ d, 0, keepdims=False)
        asked[d] = swap(jnp.concatenate([lists, mine.reshape(-1, LANES)]), "neg", d)
    query_blocks = [queries]
    for d in range(1, n_qry):
        query_blocks.append(swap(queries, "qry", d))

    base = (own_neg * cap).astype(jnp.int32).reshape(1)
    wanted = jnp.concatenate([asked[d][(half + 1) * groups :].reshape(cap) for d in far])
    rows, wm, ws, wn = gather_rows(
        wanted, cap, items_table, (message_weight, self_weight, neighbour_weight)
    )
    parts = []
    for j, d in enumerate(far):
        part = partial_hidden(
            base, rows, j, asked[d], (negatives, neighbours), wm, message_bias[:, None], ws, wn
        )
        base, part = lax.optimization_barrier((base, part))
        parts.append(swap(part, "neg", d))

    count = lax.dynamic_slice_in_dim(negative_count, own_qry * negatives, negatives)
    negative_embed, peak, total = embed_and_score(
        parts, query_blocks, output_bias[:, None], count[:, None]
    )
    pairs = jnp.stack([peak, total], axis=1)
    pairs = jnp.stack([swap(pairs[d], "qry", d) for d in range(n_qry)])
    pairs = lax.all_gather(pairs, "neg").reshape(n_neg * n_qry, 2, -1)
    top = jnp.max(pairs[:, 0], axis=0)
    whole = jnp.sum(pairs[:, 1] * jnp.exp(pairs[:, 0] - top[None, :]), axis=0)
    query_lse = top + jnp.log(whole) - math.log(negatives * n_neg * n_qry)
    return (negative_embed, query_lse)


def solution(mesh):
    in_specs = (
        P("neg", None),
        P(("neg", "qry"), None),
        P(("neg", "qry"), None),
        P(("neg", "qry")),
        P(("neg", "qry")),
        P("neg"),
        P(),
        P(),
        P(),
        P(),
        P(),
        P("qry", None),
    )
    out_specs = (P(("neg", "qry"), None), P("qry"))
    return jax.shard_map(
        per_device, mesh=mesh, in_specs=in_specs, out_specs=out_specs, check_vma=False
    )
```
